32 devices in a mesh: wide: 4 (over y, x), narrow: 8 (over z, core).
Axes of the slice: x: 2, y: 2, z: 4, core: 2. Of those that a mesh axis runs over, the one named last changes fastest.
Arguments:
- amplitudes: bfloat16 [1024, 65536], P('narrow', 'wide'), may hold values from -6 to 6
- ladder_ints: bfloat16 [65536, 8192], P('wide', 'narrow'), may hold values from -0.0234375 to 0.0234375
- cycle_amps: bfloat16 [1024, 8192], P('wide', 'narrow'), may hold values from -6 to 6
- cycle_ints: bfloat16 [8192, 8192], P('narrow', 'wide'), may hold values from -0.0625 to 0.0625
Outputs:
- residual: bfloat16 [32, 32, 32, 256], P('wide', None, 'narrow')
The draws below stay inside these ranges and needn't reach their ends.
All inputs are finite; a program needn't handle non-finite values.
Results may differ from the reference program's by a relative error of at most 0.001.
Values may be sent and summed in bfloat16 or wider, within the bound.
A program may use at most 128 MiB of HBM per device.

```python
import jax
import jax.numpy as jnp

OCC = 32
VIRT = 256
WINDOW = 32


def block_levels(own_key, extent, shards, least, top_value):
    loudness, own = 1.0, jax.random.fold_in(own_key, 6)
    for position, blocks in shards:
        steps = jnp.exp(jax.random.uniform(jax.random.fold_in(own, position), (blocks,), jnp.float32, least / len(shards), top_value / len(shards)))
        loudness = loudness * jnp.repeat(steps, extent[position] // blocks).reshape([-1 if axis == position else 1 for axis in range(len(extent))])
    return loudness


def centred(stream_key, dims, deviation, limit, shards=(), dtype=jnp.bfloat16):
    entries = jax.random.normal(stream_key, dims, jnp.float32) * deviation
    if len(shards) > 0:
        entries = block_levels(stream_key, dims, shards, -0.22, 0.18) * entries
    return jnp.clip(entries, min=-limit, max=limit).astype(dtype)


def setup_inputs(seed: int = 0) -> dict:
    seeds = jax.random.split(jax.random.key(seed), 5)
    amplitudes = centred(seeds[0], (OCC * OCC, VIRT * VIRT), 1.0, 6.0, ((0, 8), (1, 4)))
    ladder_ints = centred(seeds[1], (VIRT * VIRT, WINDOW * VIRT), (VIRT * VIRT) ** -0.5, 0.0234375, ((0, 4), (1, 8)))
    cycle_amps = centred(seeds[2], (OCC * WINDOW, OCC * VIRT), 1.0, 6.0, ((0, 4), (1, 8)))
    cycle_ints = centred(seeds[3], (OCC * VIRT, OCC * VIRT), (OCC * VIRT) ** -0.5, 0.0625, ((0, 8), (1, 4)))
    return {"amplitudes": amplitudes, "ladder_ints": ladder_ints, "cycle_amps": cycle_amps, "cycle_ints": cycle_ints}


def reference(amplitudes, ladder_ints, cycle_amps, cycle_ints):
    ladder = jnp.dot(amplitudes, ladder_ints, preferred_element_type=jnp.float32)
    ladder = ladder.reshape(OCC, OCC, WINDOW, VIRT)
    cycle = jnp.dot(cycle_amps, cycle_ints, preferred_element_type=jnp.float32)
    cycle = cycle.reshape(OCC, WINDOW, OCC, VIRT)
    total = ladder + jnp.transpose(cycle, (2, 0, 1, 3))
    return total.astype(jnp.bfloat16)
```

```python
import jax
import jax.numpy as jnp
from jax import lax
from jax.sharding import PartitionSpec as P

OCC = 32
VIRT = 256
WINDOW = 32
CHUNKS = 4


def gather_rows(block, axis, size):
    if size > 4:
        return lax.all_gather(block, axis, axis=1)
    me = lax.axis_index(axis)
    shape = (block.shape[0], size) + block.shape[1:]
    out = jnp.zeros(shape, block.dtype)
    out = lax.dynamic_update_slice_in_dim(out, block[:, None], me, 1)
    for shift in range(1, size):
        pairs = [(d, (d + shift) % size) for d in range(size)]
        got = lax.ppermute(block, axis, pairs)
        out = lax.dynamic_update_slice_in_dim(out, got[:, None], lax.rem(me + size - shift, size), 1)
    return out


def scatter_sum(partial, axis, size, low_first):
    bits = size.bit_length() - 1
    me = lax.axis_index(axis)
    rows, cols = partial.shape
    held = partial.reshape((2,) * bits + (rows // size, cols))
    left = list(range(bits - 1, -1, -1))
    for bit in list(range(bits)) if low_first else list(range(bits - 1, -1, -1)):
        where = left.index(bit)
        left.remove(bit)
        mine = lax.rem(lax.div(me, 1 << bit), 2)
        keep = lax.dynamic_index_in_dim(held, mine, where, keepdims=False)
        send = lax.dynamic_index_in_dim(held, 1 - mine, where, keepdims=False)
        held = keep + lax.ppermute(send, axis, [(d, d ^ (1 << bit)) for d in range(size)])
    return held


def solution(mesh):
    wide, narrow = mesh.shape["wide"], mesh.shape["narrow"]

    def per_device(amplitudes, ladder_ints, cycle_amps, cycle_ints):
        window_local = ladder_ints.shape[1] // VIRT
        occ_rows = amplitudes.shape[0] // OCC
        occ_local = cycle_ints.shape[1] // VIRT
        chunks = min(CHUNKS, occ_rows)
        rows = amplitudes.shape[0] // chunks
        per_chunk = occ_rows // chunks

        depth = cycle_amps.shape[1]
        local = cycle_amps.reshape(-1, narrow, window_local, depth)
        local = jnp.transpose(local, (1, 0, 2, 3)).reshape(narrow, -1, depth)
        everyone = gather_rows(local, "wide", wide).reshape(-1, depth)

        gathered = []
        for c in range(chunks):
            block = amplitudes[c * rows : (c + 1) * rows]
            gathered.append(lax.all_gather(block, "narrow", axis=0, tiled=True))

        cycle = jnp.dot(everyone, cycle_ints, preferred_element_type=jnp.float32)
        cycle = lax.psum_scatter(cycle, "narrow", scatter_dimension=0, tiled=True)

        pieces = []
        for c in range(chunks):
            ladder = jnp.dot(gathered[c], ladder_ints, preferred_element_type=jnp.float32)
            half = ladder.shape[1] // 2
            if wide & (wide - 1) or narrow % wide or half % VIRT:
                piece = lax.psum_scatter(ladder, "wide", scatter_dimension=0, tiled=True)
            else:
                piece = jnp.concatenate(
                    [
                        scatter_sum(ladder[:, :half], "wide", wide, False),
                        scatter_sum(ladder[:, half:], "wide", wide, True),
                    ],
                    axis=1,
                )
            pieces.append(piece.reshape(narrow // wide, per_chunk, OCC, window_local, VIRT))
        ladder = jnp.stack(pieces, axis=1).reshape(occ_local, OCC, window_local, VIRT)
        cycle = cycle.reshape(OCC, window_local, occ_local, VIRT)
        total = ladder + jnp.transpose(cycle, (2, 0, 1, 3))
        return total.astype(jnp.bfloat16)

    in_specs = (P("narrow", "wide"), P("wide", "narrow"), P("wide", "narrow"), P("narrow", "wide"))
    out_specs = P("wide", None, "narrow", None)
    return jax.shard_map(
        per_device, mesh=mesh, in_specs=in_specs, out_specs=out_specs, check_vma=False
    )
```
